128 devices in a mesh: blk: 128 (over y, x, z, core).
Axes of the slice: x: 4, y: 4, z: 4, core: 2. Of those that a mesh axis runs over, the one named last changes fastest.
Arguments:
- node_latent: bfloat16 [524288, 128], P('blk'), may hold values from -16 to 16
- edge_latent: bfloat16 [3145728, 128], P('blk'), may hold values from -6 to 6
- edge_ends: int32 [2, 3145728], P(None, 'blk'), may hold values from 0 to 5631, as said below
- edge_owned: int32 [3145728], P('blk'), may hold values from 0 to 1, as said below
- send_index: int32 [128, 6, 256], P('blk'), may hold values from 0 to 4095, as said below
- edge_w1: bfloat16 [2, 384, 128], replicated, may hold values from -0.3125 to 0.3125
- edge_b1: float32 [2, 128], replicated, may hold values from -3 to 3
- edge_w2: bfloat16 [2, 128, 128], replicated, may hold values from -0.5 to 0.5
- edge_gain: float32 [2, 128], replicated, may hold values from 0.5 to 1.5
- edge_shift: float32 [2, 128], replicated, may hold values from -2 to 2
- node_w1: bfloat16 [2, 256, 128], replicated, may hold values from -0.375 to 0.375
- node_b1: float32 [2, 128], replicated, may hold values from -3 to 3
- node_w2: bfloat16 [2, 128, 128], replicated, may hold values from -0.5 to 0.5
- node_gain: float32 [2, 128], replicated, may hold values from 0.5 to 1.5
- node_shift: float32 [2, 128], replicated, may hold values from -2 to 2
Outputs:
- node_out: bfloat16 [524288, 128], P('blk')
- edge_out: bfloat16 [3145728, 128], P('blk')
The draws below stay inside these ranges and needn't reach their ends.
Inputs may be any that keep to these rules, and one draw needn't show every extreme that they name: edge_ends[0] holds each slot's sender, edge_ends[1] its receiver, as entries of the block's extended node list. Slot s of a block lies in tile t = s // 128; each of its ends is either an own node from (t // 6) * 128 to (t // 6 + 1) * 128 - 1 or a halo entry from 4096 + (t % 6) * 256 to 4096 + (t % 6 + 1) * 256 - 1; at most one end of a slot is a halo entry. `edge_owned`: in each block the slots with 1 come first; every block has at least 15360 of them. send_index[b, k] lists 256 distinct nodes of block b.
All inputs are finite; a program needn't handle non-finite values.
Results may differ from the reference program's by a relative error of at most 0.0085.
Values may be sent and summed in bfloat16 or wider, within the bound.
No kernel may reach another device: no remote copies, remote signals or barrier semaphores. Data moves between devices by JAX's collectives and lax.ppermute only.
A program may use at most 128 MiB of HBM per device.

```python
import jax
import jax.numpy as jnp
from jax import lax

LATENT = 128
NODE_DEV = 4096
HALO = 256
LAYERS = 2
FACES = 6
GX = 4
GY = 4
EDGE_TILE = 128
EDGE_DEV = 24576
EDGES = 3145728
N_BLK = 128


def draw_node_latent(key, part):
    total_rows = NODE_DEV * N_BLK
    position = jnp.arange(total_rows, dtype=jnp.float32)[:, None] / (total_rows - 1)
    values = jnp.clip(jax.random.normal(key, (total_rows, LATENT), jnp.float32), -5.0, 5.0)
    scales = 1.0 + 2.0 * position
    return (values * scales).astype(jnp.bfloat16)


def draw_edge_ends(key, part):
    total_slots = EDGE_DEV * N_BLK
    subkeys = jax.random.split(jax.random.fold_in(key, 11), 4)
    slot = jnp.arange(total_slots, dtype=jnp.int32) % EDGE_DEV
    tile_id = slot // EDGE_TILE
    own_base = tile_id // FACES * EDGE_TILE
    halo_base = NODE_DEV + tile_id % FACES * HALO
    categories = jax.random.randint(subkeys[0], (total_slots,), 0, 8)
    first_local = jax.random.randint(subkeys[1], (total_slots,), 0, EDGE_TILE)
    step_by = jax.random.randint(subkeys[2], (total_slots,), 1, EDGE_TILE)
    second_local = (first_local + step_by) % EDGE_TILE
    remote = halo_base + jax.random.randint(subkeys[3], (total_slots,), 0, HALO)
    senders = jnp.where(categories < 2, remote, own_base + first_local)
    receivers = jnp.where((categories >= 2) & (categories < 4), remote, own_base + second_local)
    return jnp.stack([senders, receivers]).astype(jnp.int32)


def draw_edge_owned(key, part):
    subkeys = jax.random.split(jax.random.fold_in(key, 17), 2)
    counts = jax.random.randint(subkeys[0], (N_BLK,), EDGE_DEV * 5 // 8, EDGE_DEV + 1)
    fullest = jax.random.randint(subkeys[1], (), 0, N_BLK)
    counts = jnp.where(jnp.arange(N_BLK) == fullest, EDGE_DEV, counts)
    slots = jnp.arange(EDGE_DEV)[None, :] < counts[:, None]
    return slots.astype(jnp.int32).reshape(-1)


def pick_rows(subkey):
    return jax.random.permutation(subkey, NODE_DEV)[:HALO]


def draw_send_index(key, part):
    subkeys = jax.random.split(jax.random.fold_in(key, 23), N_BLK * FACES)
    picked = jax.vmap(pick_rows)(subkeys)
    return picked.reshape(N_BLK, FACES, HALO).astype(jnp.int32)


def steps_of(rng, extent, cuts, least, high):
    loudness, own = 1.0, jax.random.fold_in(rng, 6)
    for dim, parts in cuts:
        steps = jnp.exp(jax.random.uniform(jax.random.fold_in(own, dim), (parts,), jnp.float32, least / len(cuts), high / len(cuts)))
        loudness = loudness * jnp.repeat(steps, extent[dim] // parts).reshape([-1 if axis == dim else 1 for axis in range(len(extent))])
    return loudness


def noise(key, shape, scale, limit, cuts=(), kind=jnp.bfloat16):
    level = steps_of(key, shape, cuts, -0.22, 0.18) if cuts else 1.0
    values = jax.random.normal(key, shape, jnp.float32) * scale * level
    return jnp.minimum(jnp.maximum(values, -limit), limit).astype(kind)


def setup_inputs(seed: int = 0) -> dict:
    arg_keys = jax.random.split(jax.random.key(seed), 16)
    node_latent = draw_node_latent(jax.random.fold_in(arg_keys[15], 71), 0)
    edge_latent = noise(arg_keys[1], (EDGES, LATENT), 1.0, 6.0, ((0, 128),))
    edge_ends = draw_edge_ends(jax.random.fold_in(arg_keys[15], 71), 0)
    edge_owned = draw_edge_owned(jax.random.fold_in(arg_keys[15], 71), 0)
    send_index = draw_send_index(jax.random.fold_in(arg_keys[15], 71), 0)
    edge_w1 = noise(arg_keys[5], (LAYERS, 3 * LATENT, LATENT), (3 * LATENT) ** -0.5, 0.3125)
    edge_b1 = noise(arg_keys[6], (LAYERS, LATENT), 0.5, 3.0, (), jnp.float32)
    edge_w2 = noise(arg_keys[7], (LAYERS, LATENT, LATENT), LATENT ** -0.5, 0.5)
    edge_gain = jnp.clip(1.0 + 0.1 * jax.random.normal(arg_keys[8], (LAYERS, LATENT), jnp.float32), 0.5, 1.5)
    edge_shift = noise(arg_keys[9], (LAYERS, LATENT), 0.3, 2.0, (), jnp.float32)
    node_w1 = noise(arg_keys[10], (LAYERS, 2 * LATENT, LATENT), (2 * LATENT) ** -0.5, 0.375)
    node_b1 = noise(arg_keys[11], (LAYERS, LATENT), 0.5, 3.0, (), jnp.float32)
    node_w2 = noise(arg_keys[12], (LAYERS, LATENT, LATENT), LATENT ** -0.5, 0.5)
    node_gain = jnp.clip(1.0 + 0.1 * jax.random.normal(arg_keys[13], (LAYERS, LATENT), jnp.float32), 0.5, 1.5)
    node_shift = noise(arg_keys[14], (LAYERS, LATENT), 0.3, 2.0, (), jnp.float32)
    return {"node_latent": node_latent, "edge_latent": edge_latent, "edge_ends": edge_ends, "edge_owned": edge_owned, "send_index": send_index, "edge_w1": edge_w1, "edge_b1": edge_b1, "edge_w2": edge_w2, "edge_gain": edge_gain, "edge_shift": edge_shift, "node_w1": node_w1, "node_b1": node_b1, "node_w2": node_w2, "node_gain": node_gain, "node_shift": node_shift}


def row_norm(mixed):
    centre = mixed - lax.optimization_barrier(jnp.mean(mixed, axis=1, keepdims=True))
    spread = lax.optimization_barrier(jnp.mean(centre * centre, axis=1, keepdims=True))
    return centre * lax.rsqrt(spread + 1e-05)

def reference(node_latent, edge_latent, edge_ends, edge_owned, send_index, edge_w1, edge_b1, edge_w2, edge_gain, edge_shift, node_w1, node_b1, node_w2, node_gain, node_shift):
    offsets = jnp.array([1, -1, GX, -GX, GX * GY, -GX * GY], dtype=jnp.int32)
    blocks = jnp.arange(N_BLK, dtype=jnp.int32)
    source = jnp.mod(blocks[:, None] - offsets[None, :], N_BLK).astype(jnp.int32)
    face_ids = jnp.arange(FACES, dtype=jnp.int32)[None, :]
    halo_nodes = source[:, :, None] * NODE_DEV + send_index[source, face_ids]
    own_nodes = blocks[:, None] * NODE_DEV + jnp.arange(NODE_DEV, dtype=jnp.int32)[None, :]
    lookup = jnp.concatenate([own_nodes, halo_nodes.reshape(N_BLK, FACES * HALO)], axis=1).astype(jnp.int32)
    ends = edge_ends.reshape(2, N_BLK, EDGE_DEV)
    senders = jnp.take_along_axis(lookup, ends[0], axis=1)
    receivers = jnp.take_along_axis(lookup, ends[1], axis=1)
    owned = edge_owned.reshape(N_BLK, EDGE_DEV).astype(jnp.float32)
    latents = node_latent
    edge_state = edge_latent.reshape(N_BLK, EDGE_DEV, LATENT)
    for layer_id in range(LAYERS):

        def edge_block(totals, item, latents=latents, layer_id=layer_id):
            block_edges, block_send, block_recv, block_owned = item
            joined = jnp.concatenate([block_edges, latents[block_send], latents[block_recv]], axis=1)
            hidden = jax.nn.relu(jnp.dot(joined, edge_w1[layer_id], preferred_element_type=jnp.float32) + edge_b1[layer_id]).astype(jnp.bfloat16)
            mixed = jnp.dot(hidden, edge_w2[layer_id], preferred_element_type=jnp.float32)
            normed = edge_gain[layer_id] * row_norm(mixed) + edge_shift[layer_id]
            edges_new = (block_edges.astype(jnp.float32) + block_owned[:, None] * normed).astype(jnp.bfloat16)
            totals = totals.at[block_recv].add(block_owned[:, None] * edges_new.astype(jnp.float32))
            return (totals, edges_new)
        start = jnp.zeros((N_BLK * NODE_DEV, LATENT), jnp.float32)
        totals, edge_state = lax.scan(edge_block, start, (edge_state, senders, receivers, owned))
        aggregate = totals.astype(jnp.bfloat16)
        node_in = jnp.concatenate([latents, aggregate], axis=1)
        node_hidden = jax.nn.relu(jnp.dot(node_in, node_w1[layer_id], preferred_element_type=jnp.float32) + node_b1[layer_id]).astype(jnp.bfloat16)
        update = jnp.dot(node_hidden, node_w2[layer_id], preferred_element_type=jnp.float32)
        centre_mean = lax.optimization_barrier(jnp.mean(update, axis=0))
        deviation = update - centre_mean
        variance = lax.optimization_barrier(jnp.mean(deviation * deviation, axis=0))
        latents = (latents.astype(jnp.float32) + node_gain[layer_id] * deviation * lax.rsqrt(variance + 1e-05) + node_shift[layer_id]).astype(jnp.bfloat16)
    return (latents, edge_state.reshape(N_BLK * EDGE_DEV, LATENT))
```

```python
import functools

import jax
import jax.numpy as jnp
from jax import lax
from jax.experimental import pallas as pl
from jax.experimental.pallas import tpu as pltpu
from jax.sharding import PartitionSpec as P

LAYERS = 2
FACES = 6
OFFSETS = (1, -1, 4, -4, 16, -16)
C = 128
NODES = 4096
HALO = 256
TILE = 128
EDGES = 24576
GROUPS = NODES // TILE
GSTEP = 2
GE = FACES * TILE
SE = GSTEP * GE
STEPS = GROUPS // GSTEP
NB = 256
BF = jnp.bfloat16
F32 = jnp.float32
FAR = -1000.0


def hot_rows(row, rows):
    n = row.shape[1]
    index = jnp.broadcast_to(row, (16, n)).astype(BF)[None]
    counter = lax.broadcasted_iota(jnp.int32, (rows, n), 0).astype(F32).astype(BF)
    counter = counter.reshape(rows // 16, 16, n)
    hot = jnp.where(counter == index, jnp.ones((), BF), jnp.zeros((), BF))
    return hot.reshape(rows, n)


def dot(a, b):
    return jnp.dot(a, b, preferred_element_type=F32)


def dot_nt(a, b):
    return lax.dot_general(a, b, (((1,), (1,)), ((), ())), preferred_element_type=F32)


def edge_kernel(moved, *refs):
    refs = list(refs)
    h_ref = refs.pop(0)
    if moved:
        upd_ref, scale_row, scale_col = refs.pop(0), refs.pop(0), refs.pop(0)
    halo = [refs.pop(0) for _ in range(FACES)]
    if moved:
        halo_upd = [refs.pop(0) for _ in range(FACES)]
    e_ref, idx_ref, wsr_ref, b_ref, we_ref, w2_ref, gain_ref, shift_ref = refs[:8]
    refs = refs[8:]
    if moved:
        h_out = refs.pop(0)
    e_out, own_out = refs.pop(0), refs.pop(0)
    halo_out = [refs.pop(0) for _ in range(FACES)]
    tab_ref, acc_ref = refs
    step = pl.program_id(0)

    @pl.when(step == 0)
    def _():
        acc_ref[...] = jnp.zeros_like(acc_ref)
        for k in range(FACES):
            ht = halo[k][...]
            if moved:
                a, b = scale_col[0], scale_col[1]
                a2 = jnp.concatenate([a, a], axis=1)
                b2 = jnp.concatenate([b, b], axis=1)
                ht = (ht.astype(F32) + halo_upd[k][...].astype(F32) * a2 + b2).astype(BF)
            t = dot(wsr_ref[...], ht)
            bias = jnp.concatenate([b_ref[...], b_ref[...]], axis=1)
            tab_ref[k, :, 0:HALO] = (t[0:C] + bias).astype(BF)
            tab_ref[k, :, HALO : 2 * HALO] = t[C : 2 * C].astype(BF)

    pre_own = []
    r_own = []
    e_t = []
    for g in range(GSTEP):
        hg = h_ref[g * TILE : (g + 1) * TILE, :]
        if moved:
            up = upd_ref[g * TILE : (g + 1) * TILE, :]
            hg = (hg.astype(F32) + up * scale_row[0:1, :] + scale_row[1:2, :]).astype(BF)
            h_out[g * TILE : (g + 1) * TILE, :] = hg
        t = dot_nt(wsr_ref[...], hg)
        ps = (t[0:C] + b_ref[...]).astype(BF)
        pr = t[C : 2 * C].astype(BF)
        lhs = jnp.concatenate([ps, pr, we_ref[...]], axis=1)
        lanes = slice(g * GE, (g + 1) * GE)
        if moved:
            et = e_ref[:, lanes]
        else:
            et = e_ref[lanes, :].T
        e_t.append(et)
        s_hot = hot_rows(idx_ref[0:1, lanes], TILE)
        r_hot = hot_rows(idx_ref[1:2, lanes], TILE)
        r_own.append(r_hot)
        pre_own.append(dot(lhs, jnp.concatenate([s_hot, r_hot, et], axis=0)))
    new = [[None] * FACES for _ in range(GSTEP)]
    for k in range(FACES):
        pieces = [slice(g * GE + k * TILE, g * GE + (k + 1) * TILE) for g in range(GSTEP)]
        s_row = jnp.concatenate([idx_ref[2:3, p] for p in pieces], axis=1)
        r_row = jnp.concatenate([idx_ref[3:4, p] for p in pieces], axis=1)
        own_row = jnp.concatenate([idx_ref[4:5, p] for p in pieces], axis=1)
        s_hot = hot_rows(s_row, HALO)
        r_hot = hot_rows(r_row, HALO)
        pre = dot(tab_ref[k], jnp.concatenate([s_hot, r_hot], axis=0))
        cut = slice(k * TILE, (k + 1) * TILE)
        pre = pre + jnp.concatenate([pre_own[g][:, cut] for g in range(GSTEP)], axis=1)
        hidden = jnp.maximum(pre, 0.0).astype(BF)
        z = dot(w2_ref[...], hidden)
        spread = jnp.sum(z * z, axis=0, keepdims=True) * (1.0 / C)
        rs = lax.rsqrt(spread + 1e-05)
        gain = jnp.concatenate([gain_ref[...]] * GSTEP, axis=1)
        shift = jnp.concatenate([shift_ref[...]] * GSTEP, axis=1)
        old = jnp.concatenate([e_t[g][:, cut] for g in range(GSTEP)], axis=1)
        value = old.astype(F32) + (z * gain) * (rs * own_row) + shift * own_row
        fresh = value.astype(BF)
        acc_ref[k] = acc_ref[k] + dot_nt(r_hot, fresh)
        for g in range(GSTEP):
            new[g][k] = fresh[:, g * TILE : (g + 1) * TILE]
    for g in range(GSTEP):
        lanes = slice(g * GE, (g + 1) * GE)
        whole = jnp.concatenate(new[g], axis=1)
        if moved:
            e_out[lanes, :] = whole.T
        else:
            e_out[:, lanes] = whole
        own_out[g * TILE : (g + 1) * TILE, :] = dot_nt(r_own[g], whole)

    @pl.when(step == STEPS - 1)
    def _():
        for k in range(FACES):
            halo_out[k][...] = acc_ref[k].astype(BF)


def full(shape):
    zeros = (0,) * len(shape)
    return pl.BlockSpec(shape, lambda i: zeros)


def edge_layer(moved, h, extra, halos, halo_upds, e, idx, weights):
    rows = pl.BlockSpec((GSTEP * TILE, C), lambda i: (i, 0))
    by_edge = pl.BlockSpec((SE, C), lambda i: (i, 0))
    by_lane = pl.BlockSpec((C, SE), lambda i: (0, i))
    args, specs = [h], [rows]
    if moved:
        upd, scale_row, scale_col = extra
        args += [upd, scale_row, scale_col]
        specs += [rows, full(scale_row.shape), full(scale_col.shape)]
    args += list(halos)
    specs += [full((C, HALO))] * FACES
    if moved:
        args += list(halo_upds)
        specs += [full((C, HALO))] * FACES
    args += [e, idx] + list(weights)
    specs += [by_lane if moved else by_edge, pl.BlockSpec((8, SE), lambda i: (0, i))]
    specs += [full(w.shape) for w in weights]
    outs, out_specs = [], []
    if moved:
        outs.append(jax.ShapeDtypeStruct((NODES, C), BF))
        out_specs.append(rows)
    outs.append(jax.ShapeDtypeStruct((EDGES, C) if moved else (C, EDGES), BF))
    out_specs.append(by_edge if moved else by_lane)
    outs.append(jax.ShapeDtypeStruct((NODES, C), F32))
    out_specs.append(rows)
    outs += [jax.ShapeDtypeStruct((HALO, C), BF)] * FACES
    out_specs += [full((HALO, C))] * FACES
    return pl.pallas_call(
        functools.partial(edge_kernel, moved),
        grid=(STEPS,),
        in_specs=specs,
        out_specs=out_specs,
        out_shape=outs,
        scratch_shapes=[
            pltpu.VMEM((FACES, C, 2 * HALO), BF),
            pltpu.VMEM((FACES, HALO, C), F32),
        ],
        name="edges",
    )(*args)


def node_kernel(send, *refs):
    refs = list(refs)
    h_ref, own_ref = refs.pop(0), refs.pop(0)
    ret = [refs.pop(0) for _ in range(FACES)]
    sidx_ref, w1_ref, b1_ref, w2_ref = refs[:4]
    upd_ref, stat_ref = refs[4], refs[5]
    sent = refs[6 : 6 + FACES] if send else None
    acc_ref = refs[6 + FACES] if send else None
    step = pl.program_id(0)

    @pl.when(step == 0)
    def _():
        stat_ref[...] = jnp.zeros_like(stat_ref)
        if send:
            acc_ref[...] = jnp.zeros_like(acc_ref)

    base = (step * NB).astype(F32)
    hots = [hot_rows(sidx_ref[k : k + 1, :] - base, NB) for k in range(FACES)]
    hot = jnp.concatenate(hots, axis=1)
    arrived = jnp.concatenate([r[...] for r in ret], axis=0)
    total = (own_ref[...] + dot(hot, arrived)).astype(BF)
    node_in = jnp.concatenate([h_ref[...], total], axis=1)
    hidden = jnp.maximum(dot(node_in, w1_ref[...]) + b1_ref[...], 0.0).astype(BF)
    update = dot(hidden, w2_ref[...])
    upd_ref[...] = update
    stat_ref[0:1, :] += jnp.sum(update, axis=0, keepdims=True)
    stat_ref[1:2, :] += jnp.sum(update * update, axis=0, keepdims=True)
    if send:
        ut = update.astype(BF).T
        for k in range(FACES):
            acc_ref[k] = acc_ref[k] + dot(ut, hots[k])

        @pl.when(step == NODES // NB - 1)
        def _():
            for k in range(FACES):
                sent[k][...] = acc_ref[k].astype(BF)


def node_layer(send, h, own, returned, sidx, weights):
    rows = pl.BlockSpec((NB, C), lambda i: (i, 0))
    outs = [jax.ShapeDtypeStruct((NODES, C), F32), jax.ShapeDtypeStruct((2, C), F32)]
    out_specs = [rows, full((2, C))]
    scratch = []
    if send:
        outs += [jax.ShapeDtypeStruct((C, HALO), BF)] * FACES
        out_specs += [full((C, HALO))] * FACES
        scratch = [pltpu.VMEM((FACES, C, HALO), F32)]
    return pl.pallas_call(
        functools.partial(node_kernel, send),
        grid=(NODES // NB,),
        in_specs=[rows, rows]
        + [full((HALO, C))] * FACES
        + [full(sidx.shape)]
        + [full(w.shape) for w in weights],
        out_specs=out_specs,
        out_shape=outs,
        scratch_shapes=scratch,
        name="nodes",
    )(h, own, *returned, sidx, *weights)


def pass_along(block, distance):
    n = lax.axis_size("blk")
    return lax.ppermute(block, "blk", [((i - distance) % n, i) for i in range(n)])


def total_over(stats):
    n = lax.axis_size("blk")
    parts = lax.all_to_all(jnp.broadcast_to(stats[None], (n,) + stats.shape), "blk", 0, 0)
    return jnp.sum(parts, axis=0)


def per_device(
    node_latent,
    edge_latent,
    edge_ends,
    edge_owned,
    send_index,
    edge_w1,
    edge_b1,
    edge_w2,
    edge_gain,
    edge_shift,
    node_w1,
    node_b1,
    node_w2,
    node_gain,
    node_shift,
):
    total_nodes = NODES * lax.axis_size("blk")
    faces = send_index[0]
    tile = jnp.arange(EDGES, dtype=jnp.int32) // TILE
    own_base = tile // FACES * TILE
    halo_base = NODES + tile % FACES * HALO
    owned = edge_owned > 0
    far = jnp.full((), FAR, F32)
    idx = jnp.stack(
        [
            (edge_ends[0] - own_base).astype(F32),
            jnp.where(owned, (edge_ends[1] - own_base).astype(F32), far),
            (edge_ends[0] - halo_base).astype(F32),
            jnp.where(owned, (edge_ends[1] - halo_base).astype(F32), far),
            edge_owned.astype(F32),
        ]
        + [jnp.zeros((EDGES,), F32)] * 3
    )
    sidx = faces.astype(F32)
    h = node_latent
    e = edge_latent
    rows = node_latent[faces.reshape(-1)].T
    halos = [
        pass_along(rows[:, k * HALO : (k + 1) * HALO], OFFSETS[k]) for k in range(FACES)
    ]
    extra = None
    halo_upds = None
    for layer in range(LAYERS):
        w1 = edge_w1[layer]
        w2 = edge_w2[layer].astype(F32)
        w2 = (w2 - jnp.mean(w2, axis=1, keepdims=True)).astype(BF).T
        wsr = jnp.concatenate([w1[C : 2 * C], w1[2 * C : 3 * C]], axis=1).T
        lanes = lambda v: jnp.broadcast_to(v[:, None], (C, C))
        weights = [
            wsr,
            lanes(edge_b1[layer]),
            w1[0:C].T,
            w2,
            lanes(edge_gain[layer]),
            lanes(edge_shift[layer]),
        ]
        moved = layer > 0
        outs = edge_layer(moved, h, extra, halos, halo_upds, e, idx, weights)
        if moved:
            h, outs = outs[0], outs[1:]
        e, own = outs[0], outs[1]
        returned = [pass_along(outs[2 + k], -OFFSETS[k]) for k in range(FACES)]
        node_weights = [node_w1[layer], node_b1[layer][None], node_w2[layer]]
        last = layer == LAYERS - 1
        outs = node_layer(not last, h, own, returned, sidx, node_weights)
        update, stats = outs[0], outs[1]
        if not last:
            halo_upds = [pass_along(outs[2 + k], OFFSETS[k]) for k in range(FACES)]
        totals = total_over(stats) / total_nodes
        mu = totals[0]
        var = jnp.maximum(totals[1] - mu * mu, 0.0)
        a = node_gain[layer] * lax.rsqrt(var + 1e-05)
        b = node_shift[layer] - a * mu
        if not last:
            extra = (update, jnp.stack([a, b]), jnp.stack([lanes(a), lanes(b)]))
    out = (h.astype(F32) + update * a + b).astype(BF)
    return (out, e)


def solution(mesh):
    shared = P()
    return jax.shard_map(
        per_device,
        mesh=mesh,
        in_specs=(
            P("blk", None),
            P("blk", None),
            P(None, "blk"),
            P("blk"),
            P("blk", None, None),
        )
        + (shared,) * 10,
        out_specs=(P("blk", None), P("blk", None)),
        check_vma=False,
    )
```

```python
import functools

import jax
import jax.numpy as jnp
from jax import lax
from jax.experimental import pallas as pl
from jax.experimental.pallas import tpu as pltpu
from jax.sharding import PartitionSpec as P

LAYERS = 2
FACES = 6
C = 128
NODES = 4096
HALO = 256
TILE = 128
EDGES = 24576
GROUPS = NODES // TILE
GSTEP = 8
LAG1 = 3
LAG2 = 6
GE = FACES * TILE
SE = GSTEP * GE
STEPS = GROUPS // GSTEP
NB = 256
NSTEP = 8
NLAG = 1
BF = jnp.bfloat16
F32 = jnp.float32
FAR = -1000.0


def hot_rows(row, rows):
    n = row.shape[1]
    index = jnp.broadcast_to(row, (16, n)).astype(BF)[None]
    counter = lax.broadcasted_iota(jnp.int32, (rows, n), 0).astype(F32).astype(BF)
    counter = counter.reshape(rows // 16, 16, n)
    hot = jnp.where(counter == index, jnp.ones((), BF), jnp.zeros((), BF))
    return hot.reshape(rows, n)


def dot(a, b):
    return jnp.dot(a, b, preferred_element_type=F32)


def dot_nt(a, b):
    return lax.dot_general(a, b, (((1,), (1,)), ((), ())), preferred_element_type=F32)


def receiver(ends_ref, owned_ref, lanes, base):
    local = (ends_ref[1:2, lanes] - base).astype(F32)
    return jnp.where(owned_ref[0:1, lanes] > 0, local, FAR)


def scale_shift(layer, total_ref, gain_ref, shift_ref):
    mu = total_ref[0:1, :]
    var = jnp.maximum(total_ref[1:2, :] - mu * mu, 0.0)
    a = gain_ref[layer : layer + 1, :] * lax.rsqrt(var + 1e-05)
    return a, shift_ref[layer : layer + 1, :] - a * mu


def edge_kernel(layer, moved, face_ref, *refs):
    refs = list(refs)
    h_ref = refs.pop(0)
    if moved:
        upd_ref, total_ref, ngain_ref, nshift_ref = [refs.pop(0) for _ in range(4)]
    halo = [refs.pop(0) for _ in range(FACES)]
    if moved:
        halo_upd = [refs.pop(0) for _ in range(FACES)]
    e_ref, ends_ref, owned_ref, w1_ref, b1_ref, w2_in, egain_ref, eshift_ref = refs[:8]
    refs = refs[8:]
    if moved:
        h_out = refs.pop(0)
    e_out, own_out = refs.pop(0), refs.pop(0)
    halo_out = [refs.pop(0) for _ in range(FACES)]
    tab_ref, acc_ref, wsr_ref, we_ref, w2_ref, col_ref, row_ref = refs
    step = pl.program_id(0)

    def column(row):
        return jnp.broadcast_to(row, (C, C)).T

    @pl.when(step == 0)
    def _():
        acc_ref[...] = jnp.zeros_like(acc_ref)
        w1 = w1_ref[0]
        wsr_ref[0:C] = w1[C : 2 * C].T
        wsr_ref[C : 2 * C] = w1[2 * C : 3 * C].T
        we_ref[...] = w1[0:C].T
        w2 = w2_in[0].astype(F32)
        w2 = w2 - jnp.sum(w2, axis=1, keepdims=True) * (1.0 / C)
        w2_ref[...] = w2.T.astype(BF)
        bias = column(b1_ref[layer : layer + 1, :])
        col_ref[0] = bias
        col_ref[1] = column(egain_ref[layer : layer + 1, :])
        col_ref[2] = column(eshift_ref[layer : layer + 1, :])
        bias2 = jnp.concatenate([bias, bias], axis=1)
        if moved:
            a, b = scale_shift(layer - 1, total_ref, ngain_ref, nshift_ref)
            row_ref[0:1, :] = a
            row_ref[1:2, :] = b
            a2 = jnp.concatenate([column(a)] * 2, axis=1)
            b2 = jnp.concatenate([column(b)] * 2, axis=1)
        for m in range(FACES):
            ht = halo[m][...].T
            if moved:
                ht = (ht.astype(F32) + halo_upd[m][...].astype(F32) * a2 + b2).astype(BF)
            t = dot(wsr_ref[...], ht)
            k = face_ref[m]
            tab_ref[k, :, 0:HALO] = (t[0:C] + bias2).astype(BF)
            tab_ref[k, :, HALO : 2 * HALO] = t[C : 2 * C].astype(BF)

    tables = []
    for g in range(GSTEP):
        hg = h_ref[g * TILE : (g + 1) * TILE, :]
        if moved:
            up = upd_ref[g * TILE : (g + 1) * TILE, :]
            hg = (hg.astype(F32) + up * row_ref[0:1, :] + row_ref[1:2, :]).astype(BF)
            h_out[g * TILE : (g + 1) * TILE, :] = hg
        t = dot_nt(wsr_ref[...], hg)
        ps = (t[0:C] + col_ref[0]).astype(BF)
        pr = t[C : 2 * C].astype(BF)
        tables.append(jnp.concatenate([ps, pr, we_ref[...]], axis=1))
    gain = jnp.concatenate([col_ref[1]] * 2, axis=1)
    shift = jnp.concatenate([col_ref[2]] * 2, axis=1)
    pre_own, old, r_own, fresh, hidden, r_halo = {}, {}, {}, {}, {}, {}

    def own_part(g, j):
        lanes = slice(g * GE + j * 2 * TILE, g * GE + (j + 1) * 2 * TILE)
        et = e_ref[:, lanes] if moved else e_ref[lanes, :].T
        base = (step * GSTEP + g) * TILE
        s_hot = hot_rows((ends_ref[0:1, lanes] - base).astype(F32), TILE)
        r_hot = hot_rows(receiver(ends_ref, owned_ref, lanes, base), TILE)
        r_own[g, j] = r_hot
        pre = dot(tables[g], jnp.concatenate([s_hot, r_hot, et], axis=0))
        for i in range(2):
            pre_own[g, 2 * j + i] = pre[:, i * TILE : (i + 1) * TILE]
            old[g, 2 * j + i] = et[:, i * TILE : (i + 1) * TILE]

    def two(row_of, p, k):
        cut = [slice(g * GE + k * TILE, g * GE + (k + 1) * TILE) for g in (2 * p, 2 * p + 1)]
        return jnp.concatenate([row_of(c) for c in cut], axis=1)

    def first(p, k):
        base = NODES + k * HALO
        s_hot = hot_rows(two(lambda c: (ends_ref[0:1, c] - base).astype(F32), p, k), HALO)
        r_hot = hot_rows(two(lambda c: receiver(ends_ref, owned_ref, c, base), p, k), HALO)
        r_halo[p, k] = r_hot
        pre = dot(tab_ref[k], jnp.concatenate([s_hot, r_hot], axis=0))
        pre = pre + jnp.concatenate([pre_own[2 * p, k], pre_own[2 * p + 1, k]], axis=1)
        hidden[p, k] = jnp.maximum(pre, 0.0).astype(BF)

    def second(p, k):
        z = dot(w2_ref[...], hidden[p, k])
        spread = jnp.sum(z * z, axis=0, keepdims=True) * (1.0 / C)
        own_row = two(lambda c: owned_ref[0:1, c].astype(F32), p, k)
        rs = lax.rsqrt(spread + 1e-05) * own_row
        before = jnp.concatenate([old[2 * p, k], old[2 * p + 1, k]], axis=1).astype(F32)
        value = (before + (z * gain) * rs + shift * own_row).astype(BF)
        fresh[p, k] = value
        for i in range(2):
            g = 2 * p + i
            lanes = slice(g * GE + k * TILE, g * GE + (k + 1) * TILE)
            if moved:
                e_out[lanes, :] = value[:, i * TILE : (i + 1) * TILE].T
            else:
                e_out[:, lanes] = value[:, i * TILE : (i + 1) * TILE]

    def third(p, k):
        acc_ref[k] = acc_ref[k] + dot_nt(r_halo[p, k], fresh[p, k])
        if k == FACES - 1:
            for i in range(2):
                g = 2 * p + i
                hot = jnp.concatenate([r_own[g, j] for j in range(3)], axis=1)
                new = jnp.concatenate(
                    [fresh[p, q][:, i * TILE : (i + 1) * TILE] for q in range(FACES)], axis=1
                )
                own_out[g * TILE : (g + 1) * TILE, :] = dot_nt(hot, new)

    units = [(p, k) for p in range(GSTEP // 2) for k in range(FACES)]
    parts = [(2 * p + i, j) for p in range(GSTEP // 2) for j in range(3) for i in range(2)]
    own_part(*parts[0])
    own_part(*parts[1])
    for t in range(len(units) + LAG2):
        if t < len(units):
            first(*units[t])
        if 0 <= t - LAG1 < len(units):
            second(*units[t - LAG1])
        if 0 <= t - LAG2:
            third(*units[t - LAG2])
        if t + 2 < len(parts):
            own_part(*parts[t + 2])

    @pl.when(step == STEPS - 1)
    def _():
        for k in range(FACES):
            halo_out[k][...] = acc_ref[face_ref[k]].astype(BF)


def full(shape):
    zeros = (0,) * len(shape)
    return pl.BlockSpec(shape, lambda i, *_: zeros)


def of_layer(shape, layer):
    return pl.BlockSpec((1,) + shape[1:], lambda i, *_: (layer, 0, 0))


def edge_layer(layer, faces, h, extra, halos, halo_upds, e, ends, owned, weights):
    moved = layer > 0
    rows = pl.BlockSpec((GSTEP * TILE, C), lambda i, *_: (i, 0))
    by_edge = pl.BlockSpec((SE, C), lambda i, *_: (i, 0))
    by_lane = pl.BlockSpec((C, SE), lambda i, *_: (0, i))
    args, specs = [h], [rows]
    if moved:
        args += list(extra)
        specs += [rows] + [full(x.shape) for x in extra[1:]]
    args += list(halos)
    specs += [full((HALO, C))] * FACES
    if moved:
        args += list(halo_upds)
        specs += [full((C, HALO))] * FACES
    args += [e, ends, owned] + list(weights)
    specs += [by_lane if moved else by_edge]
    specs += [pl.BlockSpec((n, SE), lambda i, *_: (0, i)) for n in (2, 1)]
    specs += [of_layer(w.shape, layer) if w.ndim == 3 else full(w.shape) for w in weights]
    outs, out_specs = [], []
    if moved:
        outs.append(jax.ShapeDtypeStruct((NODES, C), BF))
        out_specs.append(rows)
    outs.append(jax.ShapeDtypeStruct((EDGES, C) if moved else (C, EDGES), BF))
    out_specs.append(by_edge if moved else by_lane)
    outs.append(jax.ShapeDtypeStruct((NODES, C), F32))
    out_specs.append(rows)
    outs += [jax.ShapeDtypeStruct((HALO, C), BF)] * FACES
    out_specs += [full((HALO, C))] * FACES
    return pl.pallas_call(
        functools.partial(edge_kernel, layer, moved),
        grid_spec=pltpu.PrefetchScalarGridSpec(
            num_scalar_prefetch=1,
            grid=(STEPS,),
            in_specs=specs,
            out_specs=out_specs,
            scratch_shapes=[
                pltpu.VMEM((FACES, C, 2 * HALO), BF),
                pltpu.VMEM((FACES, HALO, C), F32),
                pltpu.VMEM((2 * C, C), BF),
                pltpu.VMEM((C, C), BF),
                pltpu.VMEM((C, C), BF),
                pltpu.VMEM((3, C, C), F32),
                pltpu.VMEM((8, C), F32),
            ],
        ),
        out_shape=outs,
        name="edges",
    )(faces, *args)


def rows_of(u):
    return slice(u * NB, (u + 1) * NB)


def node_kernel(layer, send, *refs):
    refs = list(refs)
    h_ref, own_ref = refs.pop(0), refs.pop(0)
    ret = [refs.pop(0) for _ in range(FACES)]
    sidx_ref, w1_ref, b1_ref, w2_ref = refs[:4]
    upd_ref, stat_ref = refs[4], refs[5]
    sent = refs[6 : 6 + FACES] if send else None
    acc_ref = refs[6 + FACES] if send else None
    sum_ref = refs[-1]
    step = pl.program_id(0)

    @pl.when(step == 0)
    def _():
        sum_ref[...] = jnp.zeros_like(sum_ref)
        if send:
            acc_ref[...] = jnp.zeros_like(acc_ref)

    arrived = jnp.concatenate([r[...] for r in ret], axis=0)
    hots, node_in, hidden, update = {}, {}, {}, {}
    sums = [jnp.zeros((8, C), F32), jnp.zeros((8, C), F32)]

    def gather(u):
        base = step * NSTEP * NB + u * NB
        hots[u] = [hot_rows((sidx_ref[k : k + 1, :] - base).astype(F32), NB) for k in range(FACES)]
        total = own_ref[rows_of(u), :] + dot(jnp.concatenate(hots[u], axis=1), arrived)
        node_in[u] = jnp.concatenate([h_ref[rows_of(u), :], total.astype(BF)], axis=1)

    def first(u):
        pre = dot(node_in[u], w1_ref[0]) + b1_ref[layer : layer + 1, :]
        hidden[u] = jnp.maximum(pre, 0.0).astype(BF)

    def second(u):
        value = dot(hidden[u], w2_ref[0])
        upd_ref[rows_of(u), :] = value
        sums[0] = sums[0] + jnp.sum(value.reshape(NB // 8, 8, C), axis=0)
        sums[1] = sums[1] + jnp.sum((value * value).reshape(NB // 8, 8, C), axis=0)
        update[u] = value.astype(BF)

    def third(u):
        if send:
            ut = update[u].T
            for k in range(FACES):
                acc_ref[k] = acc_ref[k] + dot(ut, hots[u][k])

    stages = (gather, first, second, third)
    for t in range(NSTEP + NLAG * 3):
        for i, stage in enumerate(stages):
            if 0 <= t - NLAG * i < NSTEP:
                stage(t - NLAG * i)
    sum_ref[0:1, :] += jnp.sum(sums[0], axis=0, keepdims=True)
    sum_ref[1:2, :] += jnp.sum(sums[1], axis=0, keepdims=True)

    @pl.when(step == NODES // NB // NSTEP - 1)
    def _():
        stat_ref[...] = jnp.broadcast_to(sum_ref[0:2, :][None], stat_ref.shape)
        if send:
            for k in range(FACES):
                sent[k][...] = acc_ref[k].astype(BF)


def node_layer(layer, send, devices, h, own, returned, sidx, weights):
    rows = pl.BlockSpec((NSTEP * NB, C), lambda i: (i, 0))
    stats = (devices, 2, C)
    outs = [jax.ShapeDtypeStruct((NODES, C), F32), jax.ShapeDtypeStruct(stats, F32)]
    out_specs = [rows, full(stats)]
    scratch = []
    if send:
        outs += [jax.ShapeDtypeStruct((C, HALO), BF)] * FACES
        out_specs += [full((C, HALO))] * FACES
        scratch = [pltpu.VMEM((FACES, C, HALO), F32)]
    return pl.pallas_call(
        functools.partial(node_kernel, layer, send),
        grid=(NODES // NB // NSTEP,),
        in_specs=[rows, rows]
        + [full((HALO, C))] * FACES
        + [full(sidx.shape)]
        + [of_layer(w.shape, layer) if w.ndim == 3 else full(w.shape) for w in weights],
        out_specs=out_specs,
        out_shape=outs,
        scratch_shapes=scratch + [pltpu.VMEM((8, C), F32)],
        name="nodes",
    )(h, own, *returned, sidx, *weights)


SLOTS = tuple((bit, side) for bit in (0, 2, 4) for side in (0, 1))


def swap(blocks):
    n = lax.axis_size("blk")
    out = []
    for block, (bit, side) in zip(blocks, SLOTS):
        step = 1 << bit
        pairs = [(i, (i + (step if (i >> bit) & 1 == side else -step)) % n) for i in range(n)]
        out.append(lax.ppermute(block, "blk", pairs))
    return out


def total_over(stats):
    return jnp.sum(lax.all_to_all(stats, "blk", 0, 0), axis=0)


def per_device(
    node_latent,
    edge_latent,
    edge_ends,
    edge_owned,
    send_index,
    edge_w1,
    edge_b1,
    edge_w2,
    edge_gain,
    edge_shift,
    node_w1,
    node_b1,
    node_w2,
    node_gain,
    node_shift,
):
    devices = lax.axis_size("blk")
    total_nodes = NODES * devices
    here = lax.axis_index("blk")
    odd = [(here >> bit) & 1 for bit in (0, 2, 4)]
    faces = jnp.stack([2 * j + 1 - (odd[j] ^ side) for j in range(3) for side in (0, 1)])
    index = send_index[0]
    sidx = jnp.concatenate(
        [
            jnp.where(odd[j] == side, index[2 * j : 2 * j + 1], index[2 * j + 1 : 2 * j + 2])
            for j in range(3)
            for side in (0, 1)
        ]
    )
    owned = edge_owned[None]
    h = node_latent
    e = edge_latent
    rows = node_latent[sidx.reshape(-1)]
    halos = swap([rows[k * HALO : (k + 1) * HALO] for k in range(FACES)])
    extra = None
    halo_upds = None
    edge_weights = (edge_w1, edge_b1, edge_w2, edge_gain, edge_shift)
    node_weights = (node_w1, node_b1, node_w2)
    for layer in range(LAYERS):
        outs = edge_layer(
            layer, faces, h, extra, halos, halo_upds, e, edge_ends, owned, edge_weights
        )
        if layer > 0:
            h, outs = outs[0], outs[1:]
        e, own = outs[0], outs[1]
        returned = swap(outs[2:])
        send = layer < LAYERS - 1
        outs = node_layer(layer, send, devices, h, own, returned, sidx, node_weights)
        update, stats = outs[0], outs[1]
        if send:
            halo_upds = swap(outs[2:])
        totals = total_over(stats) / total_nodes
        extra = (update, totals, node_gain, node_shift)
    a, b = scale_shift(LAYERS - 1, totals, node_gain, node_shift)
    out = (h.astype(F32) + update * a + b).astype(BF)
    return (out, e)


def solution(mesh):
    shared = P()
    return jax.shard_map(
        per_device,
        mesh=mesh,
        in_specs=(
            P("blk", None),
            P("blk", None),
            P(None, "blk"),
            P("blk"),
            P("blk", None, None),
        )
        + (shared,) * 10,
        out_specs=(P("blk", None), P("blk", None)),
        check_vma=False,
    )
```

```python
import functools

import jax
import jax.numpy as jnp
from jax import lax
from jax.experimental import pallas as pl
from jax.experimental.pallas import tpu as pltpu
from jax.sharding import PartitionSpec as P


LAYERS = 2
FACES = 6
C = 128
NODES = 4096
HALO = 256
TILE = 128
EDGES = 24576
GROUPS = NODES // TILE
GSTEP = 8
LAG1 = 3
LAG2 = 6
GE = FACES * TILE
SE = GSTEP * GE
STEPS = GROUPS // GSTEP
NB = 256
NSTEP = 8
NLAG = 1
BF = jnp.bfloat16
F32 = jnp.float32
FAR = -1000.0


def hot_rows(row, rows):
    n = row.shape[1]
    index = jnp.broadcast_to(row, (16, n)).astype(BF)[None]
    counter = lax.broadcasted_iota(jnp.int32, (rows, n), 0).astype(F32).astype(BF)
    counter = counter.reshape(rows // 16, 16, n)
    hot = jnp.where(counter == index, jnp.ones((), BF), jnp.zeros((), BF))
    return hot.reshape(rows, n)


def dot(a, b):
    return jnp.dot(a, b, preferred_element_type=F32)


def dot_nt(a, b):
    return lax.dot_general(a, b, (((1,), (1,)), ((), ())), preferred_element_type=F32)


def receiver(ends_ref, owned_ref, lanes, base):
    local = (ends_ref[1:2, lanes] - base).astype(F32)
    return jnp.where(owned_ref[0:1, lanes] > 0, local, FAR)


def scale_shift(layer, total_ref, gain_ref, shift_ref):
    mu = total_ref[0:1, :]
    var = jnp.maximum(total_ref[1:2, :] - mu * mu, 0.0)
    a = gain_ref[layer : layer + 1, :] * lax.rsqrt(var + 1e-05)
    return a, shift_ref[layer : layer + 1, :] - a * mu


def edge_kernel(layer, moved, face_ref, *refs):
    refs = list(refs)
    h_ref = refs.pop(0)
    if moved:
        upd_ref, total_ref, ngain_ref, nshift_ref = [refs.pop(0) for _ in range(4)]
    halo = [refs.pop(0) for _ in range(FACES)]
    if moved:
        halo_upd = [refs.pop(0) for _ in range(FACES)]
    e_ref, ends_ref, owned_ref, w1_ref, b1_ref, w2_in, egain_ref, eshift_ref = refs[:8]
    refs = refs[8:]
    if moved:
        h_out = refs.pop(0)
    e_out, own_out = refs.pop(0), refs.pop(0)
    halo_out = [refs.pop(0) for _ in range(FACES)]
    tab_ref, acc_ref, wsr_ref, we_ref, w2_ref, col_ref, row_ref = refs
    step = pl.program_id(0)

    def column(row):
        return jnp.broadcast_to(row, (C, C)).T

    @pl.when(step == 0)
    def _():
        acc_ref[...] = jnp.zeros_like(acc_ref)
        w1 = w1_ref[0]
        wsr_ref[0:C] = w1[C : 2 * C].T
        wsr_ref[C : 2 * C] = w1[2 * C : 3 * C].T
        we_ref[...] = w1[0:C].T
        w2 = w2_in[0].astype(F32)
        w2 = w2 - jnp.sum(w2, axis=1, keepdims=True) * (1.0 / C)
        w2_ref[...] = w2.T.astype(BF)
        bias = column(b1_ref[layer : layer + 1, :])
        col_ref[0] = bias
        col_ref[1] = column(egain_ref[layer : layer + 1, :])
        col_ref[2] = column(eshift_ref[layer : layer + 1, :])
        bias2 = jnp.concatenate([bias, bias], axis=1)
        if moved:
            a, b = scale_shift(layer - 1, total_ref, ngain_ref, nshift_ref)
            row_ref[0:1, :] = a
            row_ref[1:2, :] = b
            a2 = jnp.concatenate([column(a)] * 2, axis=1)
            b2 = jnp.concatenate([column(b)] * 2, axis=1)
        for m in range(FACES):
            ht = halo[m][...].T
            if moved:
                ht = (ht.astype(F32) + halo_upd[m][...].astype(F32) * a2 + b2).astype(BF)
            t = dot(wsr_ref[...], ht)
            k = face_ref[m]
            tab_ref[k, :, 0:HALO] = (t[0:C] + bias2).astype(BF)
            tab_ref[k, :, HALO : 2 * HALO] = t[C : 2 * C].astype(BF)

    tables = []
    for g in range(GSTEP):
        hg = h_ref[g * TILE : (g + 1) * TILE, :]
        if moved:
            up = upd_ref[g * TILE : (g + 1) * TILE, :].astype(F32)
            hg = (hg.astype(F32) + up * row_ref[0:1, :] + row_ref[1:2, :]).astype(BF)
            h_out[g * TILE : (g + 1) * TILE, :] = hg
        t = dot_nt(wsr_ref[...], hg)
        ps = (t[0:C] + col_ref[0]).astype(BF)
        pr = t[C : 2 * C].astype(BF)
        tables.append(jnp.concatenate([ps, pr, we_ref[...]], axis=1))
    gain = jnp.concatenate([col_ref[1]] * 2, axis=1)
    shift = jnp.concatenate([col_ref[2]] * 2, axis=1)
    pre_own, old, r_own, fresh, hidden, r_halo = {}, {}, {}, {}, {}, {}

    def own_part(g, j):
        lanes = slice(g * GE + j * 2 * TILE, g * GE + (j + 1) * 2 * TILE)
        et = e_ref[:, lanes] if moved else e_ref[lanes, :].T
        base = (step * GSTEP + g) * TILE
        s_hot = hot_rows((ends_ref[0:1, lanes] - base).astype(F32), TILE)
        r_hot = hot_rows(receiver(ends_ref, owned_ref, lanes, base), TILE)
        r_own[g, j] = r_hot
        pre = dot(tables[g], jnp.concatenate([s_hot, r_hot, et], axis=0))
        for i in range(2):
            pre_own[g, 2 * j + i] = pre[:, i * TILE : (i + 1) * TILE]
            old[g, 2 * j + i] = et[:, i * TILE : (i + 1) * TILE]

    def two(row_of, p, k):
        cut = [slice(g * GE + k * TILE, g * GE + (k + 1) * TILE) for g in (2 * p, 2 * p + 1)]
        return jnp.concatenate([row_of(c) for c in cut], axis=1)

    def first(p, k):
        base = NODES + k * HALO
        s_hot = hot_rows(two(lambda c: (ends_ref[0:1, c] - base).astype(F32), p, k), HALO)
        r_hot = hot_rows(two(lambda c: receiver(ends_ref, owned_ref, c, base), p, k), HALO)
        r_halo[p, k] = r_hot
        pre = dot(tab_ref[k], jnp.concatenate([s_hot, r_hot], axis=0))
        pre = pre + jnp.concatenate([pre_own[2 * p, k], pre_own[2 * p + 1, k]], axis=1)
        hidden[p, k] = jnp.maximum(pre, 0.0).astype(BF)

    def second(p, k):
        z = dot(w2_ref[...], hidden[p, k])
        spread = jnp.sum(z * z, axis=0, keepdims=True) * (1.0 / C)
        own_row = two(lambda c: owned_ref[0:1, c].astype(F32), p, k)
        rs = lax.rsqrt(spread + 1e-05) * own_row
        before = jnp.concatenate([old[2 * p, k], old[2 * p + 1, k]], axis=1).astype(F32)
        value = (before + (z * gain) * rs + shift * own_row).astype(BF)
        fresh[p, k] = value
        for i in range(2):
            g = 2 * p + i
            lanes = slice(g * GE + k * TILE, g * GE + (k + 1) * TILE)
            if moved:
                e_out[lanes, :] = value[:, i * TILE : (i + 1) * TILE].T
            else:
                e_out[:, lanes] = value[:, i * TILE : (i + 1) * TILE]

    def third(p, k):
        acc_ref[k] = acc_ref[k] + dot_nt(r_halo[p, k], fresh[p, k])
        if k == FACES - 1:
            for i in range(2):
                g = 2 * p + i
                hot = jnp.concatenate([r_own[g, j] for j in range(3)], axis=1)
                new = jnp.concatenate(
                    [fresh[p, q][:, i * TILE : (i + 1) * TILE] for q in range(FACES)], axis=1
                )
                own_out[g * TILE : (g + 1) * TILE, :] = dot_nt(hot, new).astype(BF)

    units = [(p, k) for p in range(GSTEP // 2) for k in range(FACES)]
    parts = [(2 * p + i, j) for p in range(GSTEP // 2) for j in range(3) for i in range(2)]
    own_part(*parts[0])
    own_part(*parts[1])
    for t in range(len(units) + LAG2):
        if t < len(units):
            first(*units[t])
        if 0 <= t - LAG1 < len(units):
            second(*units[t - LAG1])
        if 0 <= t - LAG2:
            third(*units[t - LAG2])
        if t + 2 < len(parts):
            own_part(*parts[t + 2])

    @pl.when(step == STEPS - 1)
    def _():
        for k in range(FACES):
            halo_out[k][...] = acc_ref[face_ref[k]].astype(BF)


def full(shape):
    zeros = (0,) * len(shape)
    return pl.BlockSpec(shape, lambda i, *_: zeros)


def of_layer(shape, layer):
    return pl.BlockSpec((1,) + shape[1:], lambda i, *_: (layer, 0, 0))


def edge_layer(layer, faces, h, extra, halos, halo_upds, e, ends, owned, weights):
    moved = layer > 0
    rows = pl.BlockSpec((GSTEP * TILE, C), lambda i, *_: (i, 0))
    by_edge = pl.BlockSpec((SE, C), lambda i, *_: (i, 0))
    by_lane = pl.BlockSpec((C, SE), lambda i, *_: (0, i))
    args, specs = [h], [rows]
    if moved:
        args += list(extra)
        specs += [rows] + [full(x.shape) for x in extra[1:]]
    args += list(halos)
    specs += [full((HALO, C))] * FACES
    if moved:
        args += list(halo_upds)
        specs += [full((C, HALO))] * FACES
    args += [e, ends, owned] + list(weights)
    specs += [by_lane if moved else by_edge]
    specs += [pl.BlockSpec((n, SE), lambda i, *_: (0, i)) for n in (2, 1)]
    specs += [of_layer(w.shape, layer) if w.ndim == 3 else full(w.shape) for w in weights]
    outs, out_specs = [], []
    if moved:
        outs.append(jax.ShapeDtypeStruct((NODES, C), BF))
        out_specs.append(rows)
    outs.append(jax.ShapeDtypeStruct((EDGES, C) if moved else (C, EDGES), BF))
    out_specs.append(by_edge if moved else by_lane)
    outs.append(jax.ShapeDtypeStruct((NODES, C), BF))
    out_specs.append(rows)
    outs += [jax.ShapeDtypeStruct((HALO, C), BF)] * FACES
    out_specs += [full((HALO, C))] * FACES
    return pl.pallas_call(
        functools.partial(edge_kernel, layer, moved),
        grid_spec=pltpu.PrefetchScalarGridSpec(
            num_scalar_prefetch=1,
            grid=(STEPS,),
            in_specs=specs,
            out_specs=out_specs,
            scratch_shapes=[
                pltpu.VMEM((FACES, C, 2 * HALO), BF),
                pltpu.VMEM((FACES, HALO, C), F32),
                pltpu.VMEM((2 * C, C), BF),
                pltpu.VMEM((C, C), BF),
                pltpu.VMEM((C, C), BF),
                pltpu.VMEM((3, C, C), F32),
                pltpu.VMEM((8, C), F32),
            ],
        ),
        out_shape=outs,
        name="edges",
    )(faces, *args)


def rows_of(u):
    return slice(u * NB, (u + 1) * NB)


def node_kernel(layer, send, *refs):
    refs = list(refs)
    h_ref, own_ref = refs.pop(0), refs.pop(0)
    ret = [refs.pop(0) for _ in range(FACES)]
    sidx_ref, w1_ref, b1_ref, w2_ref = refs[:4]
    upd_ref, stat_ref = refs[4], refs[5]
    sent = refs[6 : 6 + FACES] if send else None
    acc_ref = refs[6 + FACES] if send else None
    sum_ref = refs[-1]
    step = pl.program_id(0)

    @pl.when(step == 0)
    def _():
        sum_ref[...] = jnp.zeros_like(sum_ref)
        if send:
            acc_ref[...] = jnp.zeros_like(acc_ref)

    arrived = jnp.concatenate([r[...] for r in ret], axis=0)
    hots, node_in, hidden, update = {}, {}, {}, {}
    sums = [jnp.zeros((8, C), F32), jnp.zeros((8, C), F32)]

    def gather(u):
        base = step * NSTEP * NB + u * NB
        hots[u] = [hot_rows((sidx_ref[k : k + 1, :] - base).astype(F32), NB) for k in range(FACES)]
        total = own_ref[rows_of(u), :].astype(F32) + dot(jnp.concatenate(hots[u], axis=1), arrived)
        node_in[u] = jnp.concatenate([h_ref[rows_of(u), :], total.astype(BF)], axis=1)

    def first(u):
        pre = dot(node_in[u], w1_ref[0]) + b1_ref[layer : layer + 1, :]
        hidden[u] = jnp.maximum(pre, 0.0).astype(BF)

    def second(u):
        value = dot(hidden[u], w2_ref[0])
        upd_ref[rows_of(u), :] = value.astype(BF)
        sums[0] = sums[0] + jnp.sum(value.reshape(NB // 8, 8, C), axis=0)
        sums[1] = sums[1] + jnp.sum((value * value).reshape(NB // 8, 8, C), axis=0)
        update[u] = value.astype(BF)

    def third(u):
        if send:
            ut = update[u].T
            for k in range(FACES):
                acc_ref[k] = acc_ref[k] + dot(ut, hots[u][k])

    stages = (gather, first, second, third)
    for t in range(NSTEP + NLAG * 3):
        for i, stage in enumerate(stages):
            if 0 <= t - NLAG * i < NSTEP:
                stage(t - NLAG * i)
    sum_ref[0:1, :] += jnp.sum(sums[0], axis=0, keepdims=True)
    sum_ref[1:2, :] += jnp.sum(sums[1], axis=0, keepdims=True)

    @pl.when(step == NODES // NB // NSTEP - 1)
    def _():
        stat_ref[...] = jnp.broadcast_to(sum_ref[0:2, :][None], stat_ref.shape)
        if send:
            for k in range(FACES):
                sent[k][...] = acc_ref[k].astype(BF)


def node_layer(layer, send, devices, h, own, returned, sidx, weights):
    rows = pl.BlockSpec((NSTEP * NB, C), lambda i: (i, 0))
    stats = (devices, 2, C)
    outs = [jax.ShapeDtypeStruct((NODES, C), BF), jax.ShapeDtypeStruct(stats, F32)]
    out_specs = [rows, full(stats)]
    scratch = []
    if send:
        outs += [jax.ShapeDtypeStruct((C, HALO), BF)] * FACES
        out_specs += [full((C, HALO))] * FACES
        scratch = [pltpu.VMEM((FACES, C, HALO), F32)]
    return pl.pallas_call(
        functools.partial(node_kernel, layer, send),
        grid=(NODES // NB // NSTEP,),
        in_specs=[rows, rows]
        + [full((HALO, C))] * FACES
        + [full(sidx.shape)]
        + [of_layer(w.shape, layer) if w.ndim == 3 else full(w.shape) for w in weights],
        out_specs=out_specs,
        out_shape=outs,
        scratch_shapes=scratch + [pltpu.VMEM((8, C), F32)],
        name="nodes",
    )(h, own, *returned, sidx, *weights)


SLOTS = tuple((bit, side) for bit in (0, 2, 4) for side in (0, 1))


def swap(blocks):
    n = lax.axis_size("blk")
    out = []
    for block, (bit, side) in zip(blocks, SLOTS):
        step = 1 << bit
        pairs = [(i, (i + (step if (i >> bit) & 1 == side else -step)) % n) for i in range(n)]
        out.append(lax.ppermute(block, "blk", pairs))
    return out


def total_over(stats):
    parts = lax.all_to_all(stats, "blk", 0, 0)
    return jnp.sum(parts, axis=0)


def per_device(
    node_latent,
    edge_latent,
    edge_ends,
    edge_owned,
    send_index,
    edge_w1,
    edge_b1,
    edge_w2,
    edge_gain,
    edge_shift,
    node_w1,
    node_b1,
    node_w2,
    node_gain,
    node_shift,
):
    devices = lax.axis_size("blk")
    total_nodes = NODES * devices
    here = lax.axis_index("blk")
    odd = [(here >> bit) & 1 for bit in (0, 2, 4)]
    faces = jnp.stack([2 * j + 1 - (odd[j] ^ side) for j in range(3) for side in (0, 1)])
    index = send_index[0]
    sidx = jnp.concatenate(
        [
            jnp.where(odd[j] == side, index[2 * j : 2 * j + 1], index[2 * j + 1 : 2 * j + 2])
            for j in range(3)
            for side in (0, 1)
        ]
    )
    owned = edge_owned[None]
    h = node_latent
    e = edge_latent
    rows = node_latent[sidx.reshape(-1)]
    halos = swap([rows[k * HALO : (k + 1) * HALO] for k in range(FACES)])
    extra = None
    halo_upds = None
    edge_weights = (edge_w1, edge_b1, edge_w2, edge_gain, edge_shift)
    node_weights = (node_w1, node_b1, node_w2)
    for layer in range(LAYERS):
        outs = edge_layer(
            layer, faces, h, extra, halos, halo_upds, e, edge_ends, owned, edge_weights
        )
        if layer > 0:
            h, outs = outs[0], outs[1:]
        e, own = outs[0], outs[1]
        returned = swap(outs[2:])
        send = layer < LAYERS - 1
        outs = node_layer(layer, send, devices, h, own, returned, sidx, node_weights)
        update, stats = outs[0], outs[1]
        if send:
            halo_upds = swap(outs[2:])
        totals = total_over(stats) / total_nodes
        extra = (update, totals, node_gain, node_shift)
    a, b = scale_shift(LAYERS - 1, totals, node_gain, node_shift)
    out = (h.astype(F32) + update.astype(F32) * a + b).astype(BF)
    return (out, e)


def solution(mesh):
    shared = P()
    return jax.shard_map(
        per_device,
        mesh=mesh,
        in_specs=(
            P("blk", None),
            P("blk", None),
            P(None, "blk"),
            P("blk"),
            P("blk", None, None),
        )
        + (shared,) * 10,
        out_specs=(P("blk", None), P("blk", None)),
        check_vma=False,
    )
```

```python
import functools

import jax
import jax.numpy as jnp
from jax import lax
from jax.experimental import pallas as pl
from jax.experimental.pallas import tpu as pltpu
from jax.sharding import PartitionSpec as P


LAYERS = 2
FACES = 6
C = 128
NODES = 4096
HALO = 256
TILE = 128
EDGES = 24576
GROUPS = NODES // TILE
GSTEP = 8
LAG1 = 3
LAG2 = 6
GE = FACES * TILE
SE = GSTEP * GE
STEPS = GROUPS // GSTEP
NB = 256
NSTEP = 8
NLAG = 1
BF = jnp.bfloat16
F32 = jnp.float32
FAR = -1000.0


def hot_rows(row, rows):
    n = row.shape[1]
    index = jnp.broadcast_to(row, (16, n)).astype(BF)[None]
    counter = lax.broadcasted_iota(jnp.int32, (rows, n), 0).astype(F32).astype(BF)
    counter = counter.reshape(rows // 16, 16, n)
    hot = jnp.where(counter == index, jnp.ones((), BF), jnp.zeros((), BF))
    return hot.reshape(rows, n)


def dot(a, b):
    return jnp.dot(a, b, preferred_element_type=F32)


def dot_nt(a, b):
    return lax.dot_general(a, b, (((1,), (1,)), ((), ())), preferred_element_type=F32)


def receiver(ends_ref, owned_ref, lanes, base):
    local = (ends_ref[1:2, lanes] - base).astype(F32)
    return jnp.where(owned_ref[0:1, lanes] > 0, local, FAR)


def scale_shift(layer, total_ref, gain_ref, shift_ref):
    count = 1.0 / (NODES * lax.axis_size("blk"))
    mu = total_ref[0:1, :] * count
    var = jnp.maximum(total_ref[1:2, :] * count - mu * mu, 0.0)
    a = gain_ref[layer : layer + 1, :] * lax.rsqrt(var + 1e-05)
    return a, shift_ref[layer : layer + 1, :] - a * mu


def edge_kernel(layer, moved, face_ref, *refs):
    refs = list(refs)
    h_ref = refs.pop(0)
    if moved:
        upd_ref, total_ref, ngain_ref, nshift_ref = [refs.pop(0) for _ in range(4)]
    halo = [refs.pop(0) for _ in range(FACES)]
    if moved:
        halo_upd = [refs.pop(0) for _ in range(FACES)]
    e_ref, ends_ref, owned_ref, w1_ref, b1_ref, w2_in, egain_ref, eshift_ref = refs[:8]
    refs = refs[8:]
    if moved:
        h_out = refs.pop(0)
    e_out, own_out = refs.pop(0), refs.pop(0)
    halo_out = [refs.pop(0) for _ in range(FACES)]
    tab_ref, acc_ref, wsr_ref, we_ref, w2_ref, col_ref, row_ref = refs
    step = pl.program_id(0)

    def column(row):
        return jnp.broadcast_to(row, (C, C)).T

    @pl.when(step == 0)
    def _():
        acc_ref[...] = jnp.zeros_like(acc_ref)
        w1 = w1_ref[0]
        wsr_ref[0:C] = w1[C : 2 * C].T
        wsr_ref[C : 2 * C] = w1[2 * C : 3 * C].T
        we_ref[...] = w1[0:C].T
        w2 = w2_in[0].astype(F32)
        w2 = w2 - jnp.sum(w2, axis=1, keepdims=True) * (1.0 / C)
        w2_ref[...] = w2.T.astype(BF)
        bias = column(b1_ref[layer : layer + 1, :])
        col_ref[0] = bias
        col_ref[1] = column(egain_ref[layer : layer + 1, :])
        col_ref[2] = column(eshift_ref[layer : layer + 1, :])
        bias2 = jnp.concatenate([bias, bias], axis=1)
        if moved:
            a, b = scale_shift(layer - 1, total_ref, ngain_ref, nshift_ref)
            row_ref[0:1, :] = a
            row_ref[1:2, :] = b
            a2 = jnp.concatenate([column(a)] * 2, axis=1)
            b2 = jnp.concatenate([column(b)] * 2, axis=1)
        for m in range(FACES):
            ht = halo[m][...].T
            if moved:
                ht = (ht.astype(F32) + halo_upd[m][...].astype(F32) * a2 + b2).astype(BF)
            t = dot(wsr_ref[...], ht)
            k = face_ref[m]
            tab_ref[k, :, 0:HALO] = (t[0:C] + bias2).astype(BF)
            tab_ref[k, :, HALO : 2 * HALO] = t[C : 2 * C].astype(BF)

    tables = []
    for g in range(GSTEP):
        hg = h_ref[g * TILE : (g + 1) * TILE, :]
        if moved:
            up = upd_ref[g * TILE : (g + 1) * TILE, :].astype(F32)
            hg = (hg.astype(F32) + up * row_ref[0:1, :] + row_ref[1:2, :]).astype(BF)
            h_out[g * TILE : (g + 1) * TILE, :] = hg
        t = dot_nt(wsr_ref[...], hg)
        ps = (t[0:C] + col_ref[0]).astype(BF)
        pr = t[C : 2 * C].astype(BF)
        tables.append(jnp.concatenate([ps, pr, we_ref[...]], axis=1))
    gain = jnp.concatenate([col_ref[1]] * 2, axis=1)
    shift = jnp.concatenate([col_ref[2]] * 2, axis=1)
    pre_own, old, r_own, fresh, hidden, r_halo = {}, {}, {}, {}, {}, {}

    def own_part(g, j):
        lanes = slice(g * GE + j * 2 * TILE, g * GE + (j + 1) * 2 * TILE)
        et = e_ref[:, lanes] if moved else e_ref[lanes, :].T
        base = (step * GSTEP + g) * TILE
        s_hot = hot_rows((ends_ref[0:1, lanes] - base).astype(F32), TILE)
        r_hot = hot_rows(receiver(ends_ref, owned_ref, lanes, base), TILE)
        r_own[g, j] = r_hot
        pre = dot(tables[g], jnp.concatenate([s_hot, r_hot, et], axis=0))
        for i in range(2):
            pre_own[g, 2 * j + i] = pre[:, i * TILE : (i + 1) * TILE]
            old[g, 2 * j + i] = et[:, i * TILE : (i + 1) * TILE]

    def two(row_of, p, k):
        cut = [slice(g * GE + k * TILE, g * GE + (k + 1) * TILE) for g in (2 * p, 2 * p + 1)]
        return jnp.concatenate([row_of(c) for c in cut], axis=1)

    def first(p, k):
        base = NODES + k * HALO
        s_hot = hot_rows(two(lambda c: (ends_ref[0:1, c] - base).astype(F32), p, k), HALO)
        r_hot = hot_rows(two(lambda c: receiver(ends_ref, owned_ref, c, base), p, k), HALO)
        r_halo[p, k] = r_hot
        pre = dot(tab_ref[k], jnp.concatenate([s_hot, r_hot], axis=0))
        pre = pre + jnp.concatenate([pre_own[2 * p, k], pre_own[2 * p + 1, k]], axis=1)
        hidden[p, k] = jnp.maximum(pre, 0.0).astype(BF)

    def second(p, k):
        z = dot(w2_ref[...], hidden[p, k])
        spread = jnp.sum(z * z, axis=0, keepdims=True) * (1.0 / C)
        own_row = two(lambda c: owned_ref[0:1, c].astype(F32), p, k)
        rs = lax.rsqrt(spread + 1e-05) * own_row
        before = jnp.concatenate([old[2 * p, k], old[2 * p + 1, k]], axis=1).astype(F32)
        value = (before + (z * gain) * rs + shift * own_row).astype(BF)
        fresh[p, k] = value
        for i in range(2):
            g = 2 * p + i
            lanes = slice(g * GE + k * TILE, g * GE + (k + 1) * TILE)
            if moved:
                e_out[lanes, :] = value[:, i * TILE : (i + 1) * TILE].T
            else:
                e_out[:, lanes] = value[:, i * TILE : (i + 1) * TILE]

    def third(p, k):
        acc_ref[k] = acc_ref[k] + dot_nt(r_halo[p, k], fresh[p, k])
        if k == FACES - 1:
            for i in range(2):
                g = 2 * p + i
                hot = jnp.concatenate([r_own[g, j] for j in range(3)], axis=1)
                new = jnp.concatenate(
                    [fresh[p, q][:, i * TILE : (i + 1) * TILE] for q in range(FACES)], axis=1
                )
                own_out[g * TILE : (g + 1) * TILE, :] = dot_nt(hot, new).astype(BF)

    units = [(p, k) for p in range(GSTEP // 2) for k in range(FACES)]
    parts = [(2 * p + i, j) for p in range(GSTEP // 2) for j in range(3) for i in range(2)]
    own_part(*parts[0])
    own_part(*parts[1])
    for t in range(len(units) + LAG2):
        if t < len(units):
            first(*units[t])
        if 0 <= t - LAG1 < len(units):
            second(*units[t - LAG1])
        if 0 <= t - LAG2:
            third(*units[t - LAG2])
        if t + 2 < len(parts):
            own_part(*parts[t + 2])

    @pl.when(step == STEPS - 1)
    def _():
        for k in range(FACES):
            halo_out[k][...] = acc_ref[face_ref[k]].astype(BF)


def full(shape):
    zeros = (0,) * len(shape)
    return pl.BlockSpec(shape, lambda i, *_: zeros)


def of_layer(shape, layer):
    return pl.BlockSpec((1,) + shape[1:], lambda i, *_: (layer, 0, 0))


def edge_layer(layer, faces, h, extra, halos, halo_upds, e, ends, owned, weights):
    moved = layer > 0
    rows = pl.BlockSpec((GSTEP * TILE, C), lambda i, *_: (i, 0))
    by_edge = pl.BlockSpec((SE, C), lambda i, *_: (i, 0))
    by_lane = pl.BlockSpec((C, SE), lambda i, *_: (0, i))
    args, specs = [h], [rows]
    if moved:
        args += list(extra)
        specs += [rows] + [full(x.shape) for x in extra[1:]]
    args += list(halos)
    specs += [full((HALO, C))] * FACES
    if moved:
        args += list(halo_upds)
        specs += [full((C, HALO))] * FACES
    args += [e, ends, owned] + list(weights)
    specs += [by_lane if moved else by_edge]
    specs += [pl.BlockSpec((n, SE), lambda i, *_: (0, i)) for n in (2, 1)]
    specs += [of_layer(w.shape, layer) if w.ndim == 3 else full(w.shape) for w in weights]
    outs, out_specs = [], []
    if moved:
        outs.append(jax.ShapeDtypeStruct((NODES, C), BF))
        out_specs.append(rows)
    outs.append(jax.ShapeDtypeStruct((EDGES, C) if moved else (C, EDGES), BF))
    out_specs.append(by_edge if moved else by_lane)
    outs.append(jax.ShapeDtypeStruct((NODES, C), BF))
    out_specs.append(rows)
    outs += [jax.ShapeDtypeStruct((HALO, C), BF)] * FACES
    out_specs += [full((HALO, C))] * FACES
    return pl.pallas_call(
        functools.partial(edge_kernel, layer, moved),
        grid_spec=pltpu.PrefetchScalarGridSpec(
            num_scalar_prefetch=1,
            grid=(STEPS,),
            in_specs=specs,
            out_specs=out_specs,
            scratch_shapes=[
                pltpu.VMEM((FACES, C, 2 * HALO), BF),
                pltpu.VMEM((FACES, HALO, C), F32),
                pltpu.VMEM((2 * C, C), BF),
                pltpu.VMEM((C, C), BF),
                pltpu.VMEM((C, C), BF),
                pltpu.VMEM((3, C, C), F32),
                pltpu.VMEM((8, C), F32),
            ],
        ),
        out_shape=outs,
        name="edges",
    )(faces, *args)


def rows_of(u):
    return slice(u * NB, (u + 1) * NB)


def node_kernel(layer, send, *refs):
    refs = list(refs)
    h_ref, own_ref = refs.pop(0), refs.pop(0)
    ret = [refs.pop(0) for _ in range(FACES)]
    sidx_ref, w1_ref, b1_ref, w2_ref = refs[:4]
    upd_ref, stat_ref = refs[4], refs[5]
    sent = refs[6 : 6 + FACES] if send else None
    acc_ref = refs[6 + FACES] if send else None
    sum_ref = refs[-1]
    step = pl.program_id(0)

    @pl.when(step == 0)
    def _():
        sum_ref[...] = jnp.zeros_like(sum_ref)
        if send:
            acc_ref[...] = jnp.zeros_like(acc_ref)

    arrived = jnp.concatenate([r[...] for r in ret], axis=0)
    hots, node_in, hidden, update = {}, {}, {}, {}
    sums = [jnp.zeros((8, C), F32), jnp.zeros((8, C), F32)]

    def gather(u):
        base = step * NSTEP * NB + u * NB
        hots[u] = [hot_rows((sidx_ref[k : k + 1, :] - base).astype(F32), NB) for k in range(FACES)]
        total = own_ref[rows_of(u), :].astype(F32) + dot(jnp.concatenate(hots[u], axis=1), arrived)
        node_in[u] = jnp.concatenate([h_ref[rows_of(u), :], total.astype(BF)], axis=1)

    def first(u):
        pre = dot(node_in[u], w1_ref[0]) + b1_ref[layer : layer + 1, :]
        hidden[u] = jnp.maximum(pre, 0.0).astype(BF)

    def second(u):
        value = dot(hidden[u], w2_ref[0])
        upd_ref[rows_of(u), :] = value.astype(BF)
        sums[0] = sums[0] + jnp.sum(value.reshape(NB // 8, 8, C), axis=0)
        sums[1] = sums[1] + jnp.sum((value * value).reshape(NB // 8, 8, C), axis=0)
        update[u] = value.astype(BF)

    def third(u):
        if send:
            ut = update[u].T
            for k in range(FACES):
                acc_ref[k] = acc_ref[k] + dot(ut, hots[u][k])

    stages = (gather, first, second, third)
    for t in range(NSTEP + NLAG * 3):
        for i, stage in enumerate(stages):
            if 0 <= t - NLAG * i < NSTEP:
                stage(t - NLAG * i)
    sum_ref[0:1, :] += jnp.sum(sums[0], axis=0, keepdims=True)
    sum_ref[1:2, :] += jnp.sum(sums[1], axis=0, keepdims=True)

    @pl.when(step == NODES // NB // NSTEP - 1)
    def _():
        stat_ref[...] = jnp.broadcast_to(sum_ref[0:2, :][None], stat_ref.shape)
        if send:
            for k in range(FACES):
                sent[k][...] = acc_ref[k].astype(BF)


def node_layer(layer, send, devices, h, own, returned, sidx, weights):
    rows = pl.BlockSpec((NSTEP * NB, C), lambda i: (i, 0))
    stats = (devices, 2, C)
    outs = [jax.ShapeDtypeStruct((NODES, C), BF), jax.ShapeDtypeStruct(stats, F32)]
    out_specs = [rows, full(stats)]
    scratch = []
    if send:
        outs += [jax.ShapeDtypeStruct((C, HALO), BF)] * FACES
        out_specs += [full((C, HALO))] * FACES
        scratch = [pltpu.VMEM((FACES, C, HALO), F32)]
    return pl.pallas_call(
        functools.partial(node_kernel, layer, send),
        grid=(NODES // NB // NSTEP,),
        in_specs=[rows, rows]
        + [full((HALO, C))] * FACES
        + [full(sidx.shape)]
        + [of_layer(w.shape, layer) if w.ndim == 3 else full(w.shape) for w in weights],
        out_specs=out_specs,
        out_shape=outs,
        scratch_shapes=scratch + [pltpu.VMEM((8, C), F32)],
        name="nodes",
    )(h, own, *returned, sidx, *weights)


SLOTS = tuple((bit, side) for bit in (0, 2, 4) for side in (0, 1))


def swap(blocks):
    n = lax.axis_size("blk")
    out = []
    for block, (bit, side) in zip(blocks, SLOTS):
        step = 1 << bit
        pairs = [(i, (i + (step if (i >> bit) & 1 == side else -step)) % n) for i in range(n)]
        out.append(lax.ppermute(block, "blk", pairs))
    return out


def total_over(stats):
    parts = lax.all_to_all(stats, "blk", 0, 0)
    return jnp.sum(parts, axis=0)


def per_device(
    node_latent,
    edge_latent,
    edge_ends,
    edge_owned,
    send_index,
    edge_w1,
    edge_b1,
    edge_w2,
    edge_gain,
    edge_shift,
    node_w1,
    node_b1,
    node_w2,
    node_gain,
    node_shift,
):
    devices = lax.axis_size("blk")
    here = lax.axis_index("blk")
    odd = [(here >> bit) & 1 for bit in (0, 2, 4)]
    faces = jnp.stack([2 * j + 1 - (odd[j] ^ side) for j in range(3) for side in (0, 1)])
    index = send_index[0]
    sidx = jnp.concatenate(
        [
            jnp.where(odd[j] == side, index[2 * j : 2 * j + 1], index[2 * j + 1 : 2 * j + 2])
            for j in range(3)
            for side in (0, 1)
        ]
    )
    owned = edge_owned[None]
    h = node_latent
    e = edge_latent
    rows = node_latent[sidx.reshape(-1)]
    halos = swap([rows[k * HALO : (k + 1) * HALO] for k in range(FACES)])
    extra = None
    halo_upds = None
    edge_weights = (edge_w1, edge_b1, edge_w2, edge_gain, edge_shift)
    node_weights = (node_w1, node_b1, node_w2)
    for layer in range(LAYERS):
        outs = edge_layer(
            layer, faces, h, extra, halos, halo_upds, e, edge_ends, owned, edge_weights
        )
        if layer > 0:
            h, outs = outs[0], outs[1:]
        e, own = outs[0], outs[1]
        returned = swap(outs[2:])
        send = layer < LAYERS - 1
        outs = node_layer(layer, send, devices, h, own, returned, sidx, node_weights)
        update, stats = outs[0], outs[1]
        if send:
            halo_upds = swap(outs[2:])
        totals = total_over(stats)
        extra = (update, totals, node_gain, node_shift)
    a, b = scale_shift(LAYERS - 1, totals, node_gain, node_shift)
    out = (h.astype(F32) + update.astype(F32) * a + b).astype(BF)
    return (out, e)


def solution(mesh):
    shared = P()
    return jax.shard_map(
        per_device,
        mesh=mesh,
        in_specs=(
            P("blk", None),
            P("blk", None),
            P(None, "blk"),
            P("blk"),
            P("blk", None, None),
        )
        + (shared,) * 10,
        out_specs=(P("blk", None), P("blk", None)),
        check_vma=False,
    )
```
